128 devices in a mesh: chip: 32 (over x, z, core), cores: 4 (over y).
Axes of the slice: x: 4, y: 4, z: 4, core: 2. Of those that a mesh axis runs over, the one named last changes fastest.
Arguments:
- start_offset: float32 [4096, 512], P(('chip', 'cores')), may hold values from -4 to 4
- chars: float32 [4096, 6, 512], P(('chip', 'cores')), may hold values from -3 to 3
- share_rel: float32 [4096, 512], P(('chip', 'cores')), may hold values from -2.5 to 2.5
- draws: float32 [4096, 6, 768], P(('chip', 'cores')), may hold values from -3 to 3
- sigma: float32 [6], replicated, may hold values from 0.1 to 0.8
- counts: int32 [4096], P(('chip', 'cores')), may hold values from 8 to 512, as said below
- converged: int32 [4096], P(('chip', 'cores')), may hold values from 0 to 1, as said below
- destination: int32 [4096], P(('chip', 'cores')), may hold values from -1 to 1535, as said below
Outputs:
- delta: float32 [4096, 512], P(('chip', 'cores'))
- work_delta: float32 [1536, 512], P(('chip', 'cores'))
- step_norm: float32 [], replicated
The draws below stay inside these ranges and needn't reach their ends.
Inputs may be any that keep to these rules, and one draw needn't show every extreme that they name: `counts`: on every device one market has exactly 512 products. On every device between 4 and 20 markets have converged 0. destination is -1 exactly where converged is 1; otherwise it is v * 12 + s with s < 12 and v a device (numbered chip-major over chip and cores) with the same cores index as the market's own device. Every device's 12 slots are each named exactly once. At most 1 markets of one device name slots of one other device, and some pair reaches that number.
All inputs are finite; a program needn't handle non-finite values.
Results may differ from the reference program's by a relative error of at most 0.0003.
Values sent between devices are 32-bit elements; how exact they have to be, the bound alone decides.
No kernel may reach another device: no remote copies, remote signals or barrier semaphores. Data moves between devices by JAX's collectives and lax.ppermute only.
A program may use at most 64 MiB of HBM per device.

```python
import math
import jax
import jax.numpy as jnp
from jax import lax

LOCAL_TRADE_ZONE = 32
PMAX = 512
K = 6
R = 768
TAIL_ITERS = 4
MARKETS = 4096
SLOTS = 12
N_CHIP = 32
N_CORES = 4
DEVICES = 128


def integer_plan(key):
    devices = N_CHIP * N_CORES
    markets = LOCAL_TRADE_ZONE * devices
    order = jnp.arange(markets, dtype=jnp.int32)
    device_of = order // LOCAL_TRADE_ZONE
    local_of = order % LOCAL_TRADE_ZONE
    chip_of = device_of // N_CORES
    core_of = device_of % N_CORES
    counts = jax.random.randint(jax.random.fold_in(key, 11), (markets,), 8, PMAX + 1, dtype=jnp.int32)
    widest = jax.random.randint(jax.random.fold_in(key, 12), (devices,), 0, LOCAL_TRADE_ZONE, dtype=jnp.int32)
    counts = jnp.where(local_of == widest[device_of], PMAX, counts).astype(jnp.int32)
    chip_line = jnp.arange(N_CHIP, dtype=jnp.int32)
    even_allotment = LOCAL_TRADE_ZONE // 8 + chip_line * (LOCAL_TRADE_ZONE // 2) // (N_CHIP - 1)
    leftover_regions = N_CHIP * (3 * LOCAL_TRADE_ZONE // 8) - jnp.sum(even_allotment)
    scores = jax.random.randint(jax.random.fold_in(key, 13), (N_CORES, N_CHIP - 1), 0, 2 ** 20, dtype=jnp.int32) * N_CHIP + chip_line[None, :N_CHIP - 1]
    accelerator_indices = jnp.argsort(jnp.argsort(scores, axis=1, stable=True), axis=1, stable=True)
    extra_allotment = (accelerator_indices < leftover_regions).astype(jnp.int32)
    extra_allotment = jnp.concatenate([extra_allotment, jnp.zeros((N_CORES, 1), jnp.int32)], axis=1)
    awaiting_regions = even_allotment[None, :] + extra_allotment
    u_of = awaiting_regions[core_of, chip_of]
    local_scores = jax.random.randint(jax.random.fold_in(key, 14), (devices, LOCAL_TRADE_ZONE), 0, 2 ** 20, dtype=jnp.int32) * LOCAL_TRADE_ZONE + jnp.arange(LOCAL_TRADE_ZONE, dtype=jnp.int32)[None, :]
    local_rank = jnp.argsort(jnp.argsort(local_scores, axis=1, stable=True), axis=1, stable=True).reshape(markets)
    moving = local_rank < u_of
    converged = jnp.where(moving, 0, 1).astype(jnp.int32)
    position = jnp.cumsum(moving.astype(jnp.int32).reshape(devices, LOCAL_TRADE_ZONE), axis=1).reshape(markets) - 1
    before = jnp.cumsum(awaiting_regions, axis=1) - awaiting_regions
    sequence = before[core_of, chip_of] + position
    shift = jax.random.randint(jax.random.fold_in(key, 15), (N_CORES,), 0, N_CHIP, dtype=jnp.int32)
    dest_chip = (sequence + shift[core_of]) % N_CHIP
    dest_slot = sequence // N_CHIP
    destination = jnp.where(moving, (dest_chip * N_CORES + core_of) * SLOTS + dest_slot, -1).astype(jnp.int32)
    return (counts, converged, destination)


def draw_counts(key, part):
    return integer_plan(key)[0]


def draw_converged(key, part):
    return integer_plan(key)[1]


def draw_destination(key, part):
    return integer_plan(key)[2]


def block_levels(key, dims, cuts, low, largest):
    def one(axis_at, parts):
        steps = jax.random.uniform(jax.random.fold_in(jax.random.fold_in(key, 6), axis_at), (parts,), jnp.float32, low / len(cuts), largest / len(cuts))
        return jnp.repeat(jnp.exp(steps), dims[axis_at] // parts).reshape((-1,) + (1,) * (len(dims) - axis_at - 1))

    gain = one(*cuts[0])
    for cut in cuts[1:]:
        gain = gain * one(*cut)
    return gain


def bell_draw(stream_key, extent, width, limit, pieces=(), kind=jnp.bfloat16):
    entries = jax.random.normal(stream_key, extent, jnp.float32) * width
    if len(pieces) > 0:
        entries = block_levels(stream_key, extent, pieces, -0.22, 0.18) * entries
    return jnp.clip(entries, min=-limit, max=limit).astype(kind)


def setup_inputs(seed: int = 0) -> dict:
    seeds = jax.random.split(jax.random.key(seed), 9)
    return {
        "start_offset": bell_draw(seeds[0], (MARKETS, PMAX), 1.0, 4.0, ((0, 128),), jnp.float32),
        "chars": bell_draw(seeds[1], (MARKETS, K, PMAX), 1.0, 3.0, ((0, 128),), jnp.float32),
        "share_rel": bell_draw(seeds[2], (MARKETS, PMAX), 0.5, 2.5, ((0, 128),), jnp.float32),
        "draws": bell_draw(seeds[3], (MARKETS, K, R), 1.0, 3.0, ((0, 128),), jnp.float32),
        "sigma": jnp.clip(jnp.exp(jax.random.uniform(seeds[4], (K,), jnp.float32, math.log(0.1), math.log(0.8))), 0.1, 0.8),
        "counts": draw_counts(jax.random.fold_in(seeds[8], 71), 0),
        "converged": draw_converged(jax.random.fold_in(seeds[8], 71), 0),
        "destination": draw_destination(jax.random.fold_in(seeds[8], 71), 0),
    }


def shock_table(features, market_draws, live_rows, coef_scale):
    spread = jnp.einsum('kj,kr->jr', features * coef_scale[:, None], market_draws, precision=lax.Precision.HIGHEST)
    return jnp.exp(spread) * live_rows[:, None]

def contract(deltas, table, log_share, live_rows):
    utility = jnp.exp(deltas)[:, None] * table
    inside = lax.optimization_barrier(jnp.sum(utility, axis=0))
    predicted = lax.optimization_barrier(jnp.mean(utility / (1.0 + inside)[None, :], axis=1))
    updated = deltas + log_share - jnp.log(jnp.where(live_rows > 0, predicted, 1.0))
    return updated * live_rows

def reference(start_offset, chars, share_rel, draws, sigma, counts, converged, destination):
    positions = jnp.arange(PMAX, dtype=jnp.int32)
    live_mask = (positions[None, :] < counts[:, None]).astype(start_offset.dtype)
    log_obs = share_rel - jnp.log(counts.astype(share_rel.dtype))[:, None] - 1.5
    initial = (log_obs + start_offset) * live_mask

    def market(packed):
        deltas, features, log_share, market_draws, live_rows = packed
        table = shock_table(features, market_draws, live_rows, sigma)
        initial_update = contract(deltas, table, log_share, live_rows)
        second = contract(initial_update, table, log_share, live_rows)
        latest = second
        for step in range(TAIL_ITERS):
            latest = contract(latest, table, log_share, live_rows)
        return (second, latest)
    second, final_step = lax.map(market, (initial, chars, log_obs, draws, live_mask))
    keep_mask = (converged == 1)[:, None]
    deltas = jnp.where(keep_mask, second, final_step)
    change = jnp.sum(jnp.where(keep_mask, 0.0, (final_step - second) ** 2))
    active = jnp.sum(jnp.where(converged == 1, 0, counts)).astype(jnp.int32)
    step_norm = jnp.sqrt(change / active.astype(change.dtype))
    slot_index = jnp.where(converged == 1, DEVICES * SLOTS, destination).astype(jnp.int32)
    work_delta = jnp.zeros((DEVICES * SLOTS, PMAX), final_step.dtype).at[slot_index].set(final_step, mode='drop')
    return (deltas, work_delta, step_norm)
```

```python
import functools
import math

import jax
import jax.numpy as jnp
from jax import lax
from jax.experimental import pallas as pl
from jax.experimental.pallas import tpu as pltpu
from jax.sharding import Mesh
from jax.sharding import PartitionSpec as P

TAIL_ITERS = 4
CHIP = ("chip_0", "chip_1", "chip_2")
CHIP_CORES = ("chip_0", "chip_1", "chip_2", "cores")

GROUP = 4
LANES = 128
LOG2E = math.log2(math.e)
LIFT = 2.0**40
BF = jnp.bfloat16
F32 = jnp.float32


def three_parts(x):
    hi = x.astype(BF).astype(F32)
    mid = (x - hi).astype(BF).astype(F32)
    return hi, mid, x - hi - mid


def hi_lo_rows(x):
    hi = x.astype(BF).astype(F32)
    row = lax.broadcasted_iota(jnp.int32, x.shape, 0)
    return jnp.where(row % 2 == 0, hi, x - hi).astype(BF)


def add_pair(y):
    return y + pltpu.roll(y, 1, 0)


def dot(a, b):
    return jnp.dot(a, b, preferred_element_type=F32)


def markets_kernel(
    sigma, counts, converged, destination, start, chars, share, draws,
    delta, send,
    order, bucket_at, a_stack, b_stack, table, table_t, log_obs, goal, first, q_two, q_last,
    *, slots, cores,
):
    total, width = start.shape
    people = draws.shape[2]
    k_count = chars.shape[1]
    tiles = width // LANES
    scale = LIFT * people

    def bucket(i):
        return converged[i] * tiles + (tiles - (counts[i] + LANES - 1) // LANES)

    for b in range(2 * tiles):
        bucket_at[b] = 0

    def tally(i, _):
        b = bucket(i)
        bucket_at[b] = bucket_at[b] + 1
        return 0

    lax.fori_loop(0, total, tally, 0)
    at = jnp.int32(0)
    for b in range(2 * tiles):
        size = bucket_at[b]
        bucket_at[b] = at
        at = at + size

    def put(i, _):
        b = bucket(i)
        order[bucket_at[b]] = i
        bucket_at[b] = bucket_at[b] + 1
        return 0

    lax.fori_loop(0, total, put, 0)

    row8 = lax.broadcasted_iota(jnp.int32, (8, width), 0)
    lane = lax.broadcasted_iota(jnp.int32, (8, width), 1)
    lives = []
    for base in range(0, total, 8):
        count = jnp.zeros((8, width), jnp.int32)
        for i in range(8):
            count = jnp.where(row8 == i, counts[base + i], count)
        live = lane < count
        lives.append(live)
        rows = pl.ds(base, 8)
        obs = share[rows, :] - jnp.log(count.astype(F32)) - 1.5
        log_obs[rows, :] = obs
        wanted = jnp.where(live, jnp.exp(obs) * scale, 0.0)
        opening = jnp.where(live, jnp.exp(obs + start[rows, :]), 0.0)
        for i in range(8):
            goal[base + i] = jnp.broadcast_to(wanted[i : i + 1], (8, width))
            first[base + i] = jnp.broadcast_to(opening[i : i + 1], (8, width))

    a_stack[...] = jnp.zeros(a_stack.shape, F32)
    b_stack[...] = jnp.zeros(b_stack.shape, F32)
    kw = lax.broadcasted_iota(jnp.int32, (k_count, width), 0)
    coef = jnp.zeros((k_count, width), F32)
    for k in range(k_count):
        coef = jnp.where(kw == k, sigma[k] * LOG2E, coef)

    def put_stack(ref, parts):
        for i, part in enumerate(parts):
            ref[8 * i : 8 * i + k_count, :] = part

    def build(n, market, g):
        a1, a2, a3 = three_parts(chars[market] * coef)
        b1, b2, b3 = three_parts(draws[market])
        put_stack(a_stack, (a1, a1, a2, a1, a2, a3))
        put_stack(b_stack, (b1, b2, b1, b3, b2, b1))
        a = a_stack[:, :n]
        b = b_stack[...]
        a_t = jnp.transpose(a, (1, 0)).astype(BF)
        b_t = jnp.transpose(b, (1, 0)).astype(BF)
        table[g, :n, :] = jnp.exp2(dot(a_t, b.astype(BF))).astype(BF)
        table_t[g, :, :n] = jnp.exp2(dot(b_t, a.astype(BF))).astype(BF)

    def run_group(n, base):
        ids = [order[base + g] for g in range(GROUP)]
        busy = [1 - converged[i] for i in ids]
        iters = 2 + TAIL_ITERS * functools.reduce(jnp.maximum, busy)

        def build_one(g, _):
            build(n, order[base + g], g)
            return 0

        lax.fori_loop(0, GROUP, build_one, 0)
        goals = [goal[i, :, :n] for i in ids]
        firsts = [first[i, :, :n] for i in ids]

        def step(it, carry):
            insides = [add_pair(dot(hi_lo_rows(carry[g]), table[g, :n, :])) for g in range(GROUP)]
            weights = [hi_lo_rows(LIFT / (1.0 + x)) for x in insides]
            out = []
            for g in range(GROUP):
                q = add_pair(dot(weights[g], table_t[g, :, :n]))
                q_two[jnp.where(it == 1, ids[g], total), :, :n] = q
                keep = jnp.logical_or(it < 2, busy[g] == 1)
                q_last[jnp.where(keep, ids[g], total), :, :n] = q
                out.append(goals[g] / q)
            return tuple(out)

        lax.fori_loop(0, iters, step, tuple(firsts))

    def one_group(j, _):
        base = j * GROUP
        size = counts[order[base]]
        for g in range(1, GROUP):
            size = jnp.maximum(size, counts[order[base + g]])
        for t in range(1, tiles + 1):

            @pl.when((size + LANES - 1) // LANES == t)
            def _():
                run_group(t * LANES, base)

        return 0

    lax.fori_loop(0, total // GROUP, one_group, 0)

    side = lax.broadcasted_iota(jnp.int32, (1, LANES), 1)
    empty = jnp.where(side == 0, float(slots), 0.0)
    for c in range(send.shape[0]):
        send[c, :, width:] = empty
    acc = jnp.zeros((8, width), F32)
    for base in range(0, total, 8):
        rows = pl.ds(base, 8)
        obs = log_obs[rows, :] + math.log(scale)
        live = lives[base // 8]
        two = q_two[base]
        last = q_last[base]
        for i in range(1, 8):
            two = jnp.where(row8 == i, q_two[base + i], two)
            last = jnp.where(row8 == i, q_last[base + i], last)
        two = jnp.where(live, obs - jnp.log(two), 0.0)
        last = jnp.where(live, obs - jnp.log(last), 0.0)
        delta[rows, :] = last
        acc = acc + (last - two) * (last - two)
        for i in range(8):

            @pl.when(converged[base + i] == 0)
            def _():
                place = destination[base + i]
                chip = place // (slots * cores)
                send[chip, :, :width] = last[i : i + 1]
                slot = (place % slots).astype(F32)
                send[chip, :, width:] = jnp.where(side == 0, slot, 0.0)

    def tally_active(i, n):
        return n + jnp.where(converged[i] == 0, counts[i], 0)

    active = lax.fori_loop(0, total, tally_active, jnp.int32(0)).astype(F32)
    change = jnp.sum(jnp.sum(acc, axis=1, keepdims=True), axis=0, keepdims=True)
    for c in range(send.shape[0]):
        row = send[c, :, width:]
        row = jnp.where(side == 1, change, row)
        send[c, :, width:] = jnp.where(side == 2, active, row)


def same_order_sum(x, axis):
    size = lax.axis_size(axis)
    here = lax.axis_index(axis)
    parts = [x] + [
        lax.ppermute(x, axis, [(i, (i + k) % size) for i in range(size)]) for k in range(1, size)
    ]
    total = 0.0
    for source in range(size):
        for k, part in enumerate(parts):
            total = total + jnp.where((here - k) % size == source, part, 0.0)
    return total


def local(start_offset, chars, share_rel, draws, sigma, counts, converged, destination):
    market_count, width = start_offset.shape
    k_count, people = draws.shape[1:]
    chip_count = lax.axis_size(CHIP)
    cores = lax.axis_size("cores")
    slots = 3 * market_count // 8
    smem = pl.BlockSpec(memory_space=pltpu.SMEM)
    vmem = pl.BlockSpec(memory_space=pltpu.VMEM)
    delta, send = pl.pallas_call(
        functools.partial(markets_kernel, slots=slots, cores=cores),
        out_shape=(
            jax.ShapeDtypeStruct((market_count, width), F32),
            jax.ShapeDtypeStruct((chip_count, 1, width + LANES), F32),
        ),
        in_specs=[smem] * 4 + [vmem] * 4,
        out_specs=(vmem,) * 2,
        scratch_shapes=[
            pltpu.SMEM((market_count,), jnp.int32),
            pltpu.SMEM((2 * width // LANES,), jnp.int32),
            pltpu.VMEM((48, width), F32),
            pltpu.VMEM((48, people), F32),
            pltpu.VMEM((GROUP, width, people), BF),
            pltpu.VMEM((GROUP, people, width), BF),
            pltpu.VMEM((market_count, width), F32),
            pltpu.VMEM((market_count, 8, width), F32),
            pltpu.VMEM((market_count, 8, width), F32),
            pltpu.VMEM((market_count + 1, 8, width), F32),
            pltpu.VMEM((market_count + 1, 8, width), F32),
        ],
        compiler_params=pltpu.CompilerParams(vmem_limit_bytes=48 * 2**20),
        name="markets",
    )(sigma, counts, converged, destination, start_offset, chars, share_rel, draws)

    values = lax.all_to_all(send, CHIP, split_axis=0, concat_axis=0, tiled=True)
    values = values.reshape(chip_count, width + LANES)
    named = jnp.arange(slots, dtype=F32)[:, None, None] == values[None, :, width : width + 1]
    work_delta = jnp.sum(jnp.where(named, values[None, :, :width], 0.0), axis=1)
    totals = same_order_sum(jnp.sum(values[:, width + 1 : width + 3], axis=0), "cores")
    return delta, work_delta, jnp.sqrt(totals[0] / totals[1])


def solution(mesh):
    finer = Mesh(
        mesh.devices.reshape(4, 4, 2, mesh.shape["cores"]), ("chip_0", "chip_1", "chip_2", "cores")
    )
    row = P(CHIP_CORES)
    return jax.shard_map(
        local,
        mesh=finer,
        in_specs=(row, row, row, row, P(), row, row, row),
        out_specs=(row, row, P()),
        check_vma=False,
    )
```

```python
import functools
import math

import jax
import jax.numpy as jnp
from jax import lax
from jax.experimental import pallas as pl
from jax.experimental.pallas import tpu as pltpu
from jax.sharding import Mesh
from jax.sharding import PartitionSpec as P

TAIL_ITERS = 4
CHIP_CORES = ("chip_0", "chip_1", "chip_2", "cores")

GROUP = 4
EARLY = 20
LANES = 128
LOG2E = math.log2(math.e)
LIFT = 2.0**40
BF = jnp.bfloat16
F32 = jnp.float32


def three_parts(x):
    hi = x.astype(BF).astype(F32)
    mid = (x - hi).astype(BF).astype(F32)
    return hi, mid, x - hi - mid


def hi_lo_rows(x):
    hi = x.astype(BF).astype(F32)
    row = lax.broadcasted_iota(jnp.int32, x.shape, 0)
    return jnp.where(row < 4, hi, x - hi).astype(BF)


def add_halves(y):
    return y + pltpu.roll(y, 4, 0)


def by_turns(a, b):
    row = lax.broadcasted_iota(jnp.int32, a.shape, 0)
    return jnp.where(row % 2 == 0, a, b)


def dot(a, b):
    return jnp.dot(a, b, preferred_element_type=F32)


def sort_markets(counts, converged, order, bucket_at, total, tiles):
    def bucket(i):
        return converged[i] * tiles + (tiles - (counts[i] + LANES - 1) // LANES)

    for b in range(2 * tiles):
        bucket_at[b] = 0

    def tally(i, active):
        b = bucket(i)
        bucket_at[b] = bucket_at[b] + 1
        return active + jnp.where(converged[i] == 0, counts[i], 0)

    active = lax.fori_loop(0, total, tally, jnp.int32(0))
    at = jnp.int32(0)
    for b in range(2 * tiles):
        size = bucket_at[b]
        bucket_at[b] = at
        at = at + size

    def put(i, _):
        b = bucket(i)
        order[bucket_at[b]] = i
        bucket_at[b] = bucket_at[b] + 1
        return 0

    lax.fori_loop(0, total, put, 0)
    return active


def early_kernel(
    sigma, counts, converged, destination, start, chars, share, draws,
    delta, send, order,
    bucket_at, *scratch, slots,
):
    total, width = start.shape
    active = sort_markets(counts, converged, order, bucket_at, total, width // LANES)
    final_rows = run_markets(
        sigma, counts, converged, start, chars, share, draws, order, *scratch, 0, EARLY
    )
    row8 = lax.broadcasted_iota(jnp.int32, (8, width), 0)
    acc = jnp.zeros((8, width), F32)
    for base in range(0, total, 8):
        two, last = final_rows(base)
        delta[pl.ds(base, 8), :] = last
        done = jnp.ones((8, width), jnp.int32)
        for i in range(8):
            done = jnp.where(row8 == i, converged[base + i], done)
        step = jnp.where(done == 0, last - two, 0.0)
        acc = acc + step * step

    change = jnp.sum(jnp.sum(acc, axis=1, keepdims=True), axis=0, keepdims=True)
    side = lax.broadcasted_iota(jnp.int32, (1, LANES), 1)
    empty = jnp.where(side == 1, change, jnp.where(side == 2, active.astype(F32), float(slots)))
    for c in range(send.shape[0]):
        send[c, :, width:] = empty
    for i in range(total):

        @pl.when(converged[i] == 0)
        def _():
            device = destination[i] // slots
            slot = (destination[i] % slots).astype(F32)
            send[device, :, :width] = delta[i : i + 1, :]
            send[device, :, width:] = jnp.where(side == 0, slot, empty)


def late_kernel(
    sigma, counts, converged, order, start, chars, share, draws, early,
    delta,
    late, *scratch,
):
    total, width = start.shape
    final_rows = run_markets(
        sigma, counts, converged, start, chars, share, draws, order, *scratch, EARLY, total
    )
    for i in range(total):
        late[order[i]] = 1 if i >= EARLY else 0
    row8 = lax.broadcasted_iota(jnp.int32, (8, width), 0)
    for base in range(0, total, 8):
        rows = pl.ds(base, 8)
        here = jnp.zeros((8, width), jnp.int32)
        for i in range(8):
            here = jnp.where(row8 == i, late[base + i], here)
        delta[rows, :] = jnp.where(here == 1, final_rows(base)[1], early[rows, :])


def run_markets(
    sigma, counts, converged, start, chars, share, draws, order,
    a_stack, b_stack, table, table_t, log_obs, goal, first, q_two, q_last,
    begin, end,
):
    total, width = start.shape
    people = draws.shape[2]
    k_count = chars.shape[1]
    tiles = width // LANES
    scale = LIFT * people

    row8 = lax.broadcasted_iota(jnp.int32, (8, width), 0)
    lane = lax.broadcasted_iota(jnp.int32, (8, width), 1)
    lives = []
    for base in range(0, total, 8):
        count = jnp.zeros((8, width), jnp.int32)
        for i in range(8):
            count = jnp.where(row8 == i, counts[base + i], count)
        live = lane < count
        lives.append(live)
        rows = pl.ds(base, 8)
        obs = share[rows, :] - jnp.log(count.astype(F32)) - 1.5
        log_obs[rows, :] = obs
        wanted = jnp.where(live, jnp.exp(obs) * scale, 0.0)
        opening = jnp.where(live, jnp.exp(obs + start[rows, :]), 0.0)
        for i in range(8):
            goal[base + i] = jnp.broadcast_to(wanted[i : i + 1], (8, width))
            first[base + i] = jnp.broadcast_to(opening[i : i + 1], (8, width))

    a_stack[...] = jnp.zeros(a_stack.shape, F32)
    b_stack[...] = jnp.zeros(b_stack.shape, F32)
    kw = lax.broadcasted_iota(jnp.int32, (k_count, width), 0)
    coef = jnp.zeros((k_count, width), F32)
    for k in range(k_count):
        coef = jnp.where(kw == k, sigma[k] * LOG2E, coef)

    def put_stack(ref, g, parts):
        for i, part in enumerate(parts):
            ref[g, 8 * i : 8 * i + k_count, :] = part

    def build(n, market, g):
        a1, a2, a3 = three_parts(chars[market] * coef)
        b1, b2, b3 = three_parts(draws[market])
        put_stack(a_stack, g, (a1, a1, a2, a1, a2, a3))
        put_stack(b_stack, g, (b1, b2, b1, b3, b2, b1))
        a_t = jnp.transpose(a_stack[g, :, :n], (1, 0)).astype(BF)
        t = jnp.exp2(dot(a_t, b_stack[g].astype(BF))).astype(BF)
        table[g, :n, :] = t
        at = (g % 2) * n
        table_t[g // 2, :, at : at + n] = jnp.transpose(t, (1, 0))

    def run_group(n, base):
        ids = [order[base + g] for g in range(GROUP)]
        busy = [1 - converged[i] for i in ids]
        iters = 2 + TAIL_ITERS * functools.reduce(jnp.maximum, busy)
        for g in range(GROUP):
            build(n, ids[g], g)
        pairs = range(GROUP // 2)
        goals = [by_turns(goal[ids[2 * p], :, :n], goal[ids[2 * p + 1], :, :n]) for p in pairs]
        firsts = [by_turns(first[ids[2 * p], :, :n], first[ids[2 * p + 1], :, :n]) for p in pairs]

        def step(it, carry):
            weights = []
            for p in pairs:
                e = hi_lo_rows(carry[p])
                inside = by_turns(dot(e, table[2 * p, :n, :]), dot(e, table[2 * p + 1, :n, :]))
                weights.append(hi_lo_rows(LIFT / (1.0 + add_halves(inside))))
            out = []
            for p in pairs:
                y = dot(weights[p], table_t[p, :, : 2 * n])
                q = add_halves(by_turns(y[:, :n], y[:, n:]))
                other = pltpu.roll(q, 1, 0)
                for g, rows in ((2 * p, by_turns(q, other)), (2 * p + 1, by_turns(other, q))):
                    q_two[jnp.where(it == 1, ids[g], total), :, :n] = rows
                    keep = jnp.logical_or(it < 2, busy[g] == 1)
                    q_last[jnp.where(keep, ids[g], total), :, :n] = rows
                out.append(goals[p] / q)
            return tuple(out)

        lax.fori_loop(0, iters, step, tuple(firsts))

    def one_group(j, _):
        base = j * GROUP
        size = counts[order[base]]
        for g in range(1, GROUP):
            size = jnp.maximum(size, counts[order[base + g]])
        for t in range(1, tiles + 1):

            @pl.when((size + LANES - 1) // LANES == t)
            def _():
                run_group(t * LANES, base)

        return 0

    lax.fori_loop(begin // GROUP, end // GROUP, one_group, 0)

    def final_rows(base):
        obs = log_obs[pl.ds(base, 8), :] + math.log(scale)
        live = lives[base // 8]
        two = q_two[base]
        last = q_last[base]
        for i in range(1, 8):
            two = jnp.where(row8 == i, q_two[base + i], two)
            last = jnp.where(row8 == i, q_last[base + i], last)
        return (
            jnp.where(live, obs - jnp.log(two), 0.0),
            jnp.where(live, obs - jnp.log(last), 0.0),
        )

    return final_rows


def scratch_for(total, width, people):
    return [
        pltpu.VMEM((GROUP, 48, width), F32),
        pltpu.VMEM((GROUP, 48, people), F32),
        pltpu.VMEM((GROUP, width, people), BF),
        pltpu.VMEM((GROUP // 2, people, 2 * width), BF),
        pltpu.VMEM((total, width), F32),
        pltpu.VMEM((total, 8, width), F32),
        pltpu.VMEM((total, 8, width), F32),
        pltpu.VMEM((total + 1, 8, width), F32),
        pltpu.VMEM((total + 1, 8, width), F32),
    ]


def early_markets(
    sigma, counts, converged, destination, start_offset, chars, share_rel, draws,
    *, devices, slots,
):
    total, width = start_offset.shape
    people = draws.shape[2]
    smem = pl.BlockSpec(memory_space=pltpu.SMEM)
    vmem = pl.BlockSpec(memory_space=pltpu.VMEM)
    return pl.pallas_call(
        functools.partial(early_kernel, slots=slots),
        out_shape=(
            jax.ShapeDtypeStruct((total, width), F32),
            jax.ShapeDtypeStruct((devices, 1, width + LANES), F32),
            jax.ShapeDtypeStruct((total,), jnp.int32),
        ),
        in_specs=[smem] * 4 + [vmem] * 4,
        out_specs=(vmem, vmem, smem),
        scratch_shapes=[pltpu.SMEM((2 * width // LANES,), jnp.int32)]
        + scratch_for(total, width, people),
        compiler_params=pltpu.CompilerParams(vmem_limit_bytes=48 * 2**20),
        name="early_markets",
    )(sigma, counts, converged, destination, start_offset, chars, share_rel, draws)


def late_markets(
    sigma, counts, converged, order, start_offset, chars, share_rel, draws, early
):
    total, width = start_offset.shape
    people = draws.shape[2]
    smem = pl.BlockSpec(memory_space=pltpu.SMEM)
    vmem = pl.BlockSpec(memory_space=pltpu.VMEM)
    rest = total - EARLY
    return pl.pallas_call(
        late_kernel,
        out_shape=jax.ShapeDtypeStruct((total, width), F32),
        in_specs=[smem] * 4 + [vmem] * 5,
        out_specs=vmem,
        scratch_shapes=[pltpu.SMEM((total,), jnp.int32)] + scratch_for(total, width, people),
        input_output_aliases={8: 0},
        compiler_params=pltpu.CompilerParams(vmem_limit_bytes=48 * 2**20),
        cost_estimate=pl.CostEstimate(
            flops=rest * width * people * 20,
            bytes_accessed=2 * 2**20,
            transcendentals=rest * width * people,
        ),
        name="late_markets",
    )(sigma, counts, converged, order, start_offset, chars, share_rel, draws, early)


def local(start_offset, chars, share_rel, draws, sigma, counts, converged, destination):
    market_count, width = start_offset.shape
    devices = lax.axis_size(CHIP_CORES)
    slots = 3 * market_count // 8
    early, send, order = early_markets(
        sigma, counts, converged, destination, start_offset, chars, share_rel, draws,
        devices=devices, slots=slots,
    )
    values = lax.all_to_all(send, CHIP_CORES, split_axis=0, concat_axis=0, tiled=True)
    delta = late_markets(
        sigma, counts, converged, order, start_offset, chars, share_rel, draws, early
    )
    values = values.reshape(devices, width + LANES)
    named = jnp.arange(slots, dtype=F32)[:, None, None] == values[None, :, width : width + 1]
    work_delta = jnp.sum(jnp.where(named, values[None, :, :width], 0.0), axis=1)
    totals = jnp.sum(values[:, width + 1 : width + 3], axis=0)
    return delta, work_delta, jnp.sqrt(totals[0] / totals[1])


def solution(mesh):
    finer = Mesh(
        mesh.devices.reshape(4, 4, 2, mesh.shape["cores"]), ("chip_0", "chip_1", "chip_2", "cores")
    )
    row = P(CHIP_CORES)
    return jax.shard_map(
        local,
        mesh=finer,
        in_specs=(row, row, row, row, P(), row, row, row),
        out_specs=(row, row, P()),
        check_vma=False,
    )
```

```python
import functools
import math

import jax
import jax.numpy as jnp
from jax import lax
from jax.experimental import pallas as pl
from jax.experimental.pallas import tpu as pltpu
from jax.sharding import Mesh
from jax.sharding import PartitionSpec as P

TAIL_ITERS = 4
CHIP_CORES = ("chip_0", "chip_1", "chip_2", "cores")

GROUP = 4
EARLY = 20
LANES = 128
LOG2E = math.log2(math.e)
LIFT = 2.0**40
BF = jnp.bfloat16
F32 = jnp.float32


def three_parts(x):
    hi = x.astype(BF).astype(F32)
    mid = (x - hi).astype(BF).astype(F32)
    return hi, mid, x - hi - mid


def hi_lo_rows(x):
    hi = x.astype(BF).astype(F32)
    row = lax.broadcasted_iota(jnp.int32, x.shape, 0)
    return jnp.where(row < 4, hi, x - hi).astype(BF)


def add_halves(y):
    return y + pltpu.roll(y, 4, 0)


def by_turns(a, b):
    row = lax.broadcasted_iota(jnp.int32, a.shape, 0)
    return jnp.where(row % 2 == 0, a, b)


def dot(a, b):
    return jnp.dot(a, b, preferred_element_type=F32)


def sort_markets(counts, converged, order, bucket_at, total, tiles):
    def bucket(i):
        return converged[i] * tiles + (tiles - (counts[i] + LANES - 1) // LANES)

    for b in range(2 * tiles):
        bucket_at[b] = 0

    def tally(i, active):
        b = bucket(i)
        bucket_at[b] = bucket_at[b] + 1
        return active + jnp.where(converged[i] == 0, counts[i], 0)

    active = lax.fori_loop(0, total, tally, jnp.int32(0))
    at = jnp.int32(0)
    for b in range(2 * tiles):
        size = bucket_at[b]
        bucket_at[b] = at
        at = at + size

    def put(i, _):
        b = bucket(i)
        order[bucket_at[b]] = i
        bucket_at[b] = bucket_at[b] + 1
        return 0

    lax.fori_loop(0, total, put, 0)
    return active


def early_kernel(
    sigma, counts, converged, destination, start, chars, share, draws,
    delta, send, order,
    bucket_at, start_here, chars_here, share_here, draws_here, copied, *scratch, slots,
):
    total, width = start.shape
    copies = [
        pltpu.make_async_copy(source, here, copied.at[i])
        for i, (source, here) in enumerate(
            ((start, start_here), (share, share_here), (chars, chars_here), (draws, draws_here))
        )
    ]
    for copy in copies:
        copy.start()

    def ready(which):
        for copy in copies[which]:
            copy.wait()

    active = sort_markets(counts, converged, order, bucket_at, total, width // LANES)
    final_rows = run_markets(
        sigma, counts, converged, start_here, chars_here, share_here, draws_here, order, *scratch,
        0, EARLY, ready,
    )
    row8 = lax.broadcasted_iota(jnp.int32, (8, width), 0)
    acc = jnp.zeros((8, width), F32)
    for base in range(0, total, 8):
        two, last = final_rows(base)
        delta[pl.ds(base, 8), :] = last
        done = jnp.ones((8, width), jnp.int32)
        for i in range(8):
            done = jnp.where(row8 == i, converged[base + i], done)
        step = jnp.where(done == 0, last - two, 0.0)
        acc = acc + step * step

    change = jnp.sum(jnp.sum(acc, axis=1, keepdims=True), axis=0, keepdims=True)
    side = lax.broadcasted_iota(jnp.int32, (1, LANES), 1)
    empty = jnp.where(side == 1, change, jnp.where(side == 2, active.astype(F32), float(slots)))
    for c in range(send.shape[0]):
        send[c, :, width:] = empty
    for i in range(total):

        @pl.when(converged[i] == 0)
        def _():
            device = destination[i] // slots
            slot = (destination[i] % slots).astype(F32)
            send[device, :, :width] = delta[i : i + 1, :]
            send[device, :, width:] = jnp.where(side == 0, slot, empty)


def late_kernel(
    sigma, counts, converged, order, start, chars, share, draws, early,
    delta,
    late, *scratch,
):
    total, width = start.shape
    final_rows = run_markets(
        sigma, counts, converged, start, chars, share, draws, order, *scratch, EARLY, total
    )
    for i in range(total):
        late[order[i]] = 1 if i >= EARLY else 0
    row8 = lax.broadcasted_iota(jnp.int32, (8, width), 0)
    for base in range(0, total, 8):
        rows = pl.ds(base, 8)
        here = jnp.zeros((8, width), jnp.int32)
        for i in range(8):
            here = jnp.where(row8 == i, late[base + i], here)
        delta[rows, :] = jnp.where(here == 1, final_rows(base)[1], early[rows, :])


def run_markets(
    sigma, counts, converged, start, chars, share, draws, order,
    chars_rows, draws_rows, a_stack, b_stack, table, table_t, log_obs, goal, first, q_two, q_last,
    begin, end, ready=lambda which: None,
):
    total, width = start.shape
    people = draws.shape[2]
    k_count = chars.shape[0]
    tiles = width // LANES
    scale = LIFT * people

    row8 = lax.broadcasted_iota(jnp.int32, (8, width), 0)
    lane = lax.broadcasted_iota(jnp.int32, (8, width), 1)
    lives = []
    ready(slice(0, 2))
    for base in range(0, total, 8):
        count = jnp.zeros((8, width), jnp.int32)
        for i in range(8):
            count = jnp.where(row8 == i, counts[base + i], count)
        live = lane < count
        lives.append(live)
        rows = pl.ds(base, 8)
        obs = share[rows, :] - jnp.log(count.astype(F32)) - 1.5
        log_obs[rows, :] = obs
        wanted = jnp.where(live, jnp.exp(obs) * scale, 0.0)
        opening = jnp.where(live, jnp.exp(obs + start[rows, :]), 0.0)
        for i in range(8):
            goal[base + i] = jnp.broadcast_to(wanted[i : i + 1], (8, width))
            first[base + i] = jnp.broadcast_to(opening[i : i + 1], (8, width))

    coef = jnp.zeros((8, width), F32)
    for k in range(k_count):
        coef = jnp.where(row8 == k, sigma[k] * LOG2E, coef)
    ready(slice(2, 4))
    for source, rows in ((chars, chars_rows), (draws, draws_rows)):
        rows[...] = jnp.zeros(rows.shape, F32)
        for k in range(k_count):
            for base in range(0, total, 8):
                for t in range(rows.shape[0]):
                    part = source[k, base : base + 8, t * LANES : (t + 1) * LANES]
                    rows[t, pl.ds(base * 8 + k, 8, stride=8), :] = part

    def put_stack(ref, g, parts):
        for i, part in enumerate(parts):
            ref[g, 8 * i : 8 * i + 8, : part.shape[1]] = part

    def build(n, market, g):
        rows = pl.ds(pl.multiple_of(market * 8, 8), 8)
        a = jnp.concatenate([chars_rows[t, rows, :] for t in range(n // LANES)], axis=1)
        b = jnp.concatenate([draws_rows[t, rows, :] for t in range(people // LANES)], axis=1)
        a1, a2, a3 = three_parts(a * coef[:, :n])
        b1, b2, b3 = three_parts(b)
        put_stack(a_stack, g, (a1, a1, a2, a1, a2, a3))
        put_stack(b_stack, g, (b1, b2, b1, b3, b2, b1))
        a_t = jnp.transpose(a_stack[g, :, :n], (1, 0)).astype(BF)
        t = jnp.exp2(dot(a_t, b_stack[g].astype(BF))).astype(BF)
        table[g, :n, :] = t
        at = (g % 2) * n
        table_t[g // 2, :, at : at + n] = jnp.transpose(t, (1, 0))

    def run_group(n, base):
        ids = [order[base + g] for g in range(GROUP)]
        busy = [1 - converged[i] for i in ids]
        trips = 1 + TAIL_ITERS // 2 * functools.reduce(jnp.maximum, busy)
        for g in range(GROUP):
            build(n, ids[g], g)
        pairs = range(GROUP // 2)
        goals = [by_turns(goal[ids[2 * p], :, :n], goal[ids[2 * p + 1], :, :n]) for p in pairs]
        firsts = [by_turns(first[ids[2 * p], :, :n], first[ids[2 * p + 1], :, :n]) for p in pairs]

        def step(state):
            weights = []
            for p in pairs:
                e = hi_lo_rows(state[p])
                inside = by_turns(dot(e, table[2 * p, :n, :]), dot(e, table[2 * p + 1, :n, :]))
                weights.append(hi_lo_rows(LIFT / (1.0 + add_halves(inside))))
            sums = []
            for p in pairs:
                y = dot(weights[p], table_t[p, :, : 2 * n])
                sums.append(add_halves(by_turns(y[:, :n], y[:, n:])))
            return sums

        def two_steps(trip, state):
            sums = step(state)
            sums = step([goals[p] / sums[p] for p in pairs])
            for p in pairs:
                q = sums[p]
                other = pltpu.roll(q, 1, 0)
                for g, rows in ((2 * p, by_turns(q, other)), (2 * p + 1, by_turns(other, q))):
                    q_two[jnp.where(trip == 0, ids[g], total), :, :n] = rows
                    keep = jnp.logical_or(trip == 0, busy[g] == 1)
                    q_last[jnp.where(keep, ids[g], total), :, :n] = rows
            return tuple(goals[p] / sums[p] for p in pairs)

        lax.fori_loop(0, trips, two_steps, tuple(firsts))

    def one_group(j, _):
        base = j * GROUP
        size = counts[order[base]]
        for g in range(1, GROUP):
            size = jnp.maximum(size, counts[order[base + g]])
        for t in range(1, tiles + 1):

            @pl.when((size + LANES - 1) // LANES == t)
            def _():
                run_group(t * LANES, base)

        return 0

    lax.fori_loop(begin // GROUP, end // GROUP, one_group, 0)

    def final_rows(base):
        obs = log_obs[pl.ds(base, 8), :] + math.log(scale)
        live = lives[base // 8]
        two = q_two[base]
        last = q_last[base]
        for i in range(1, 8):
            two = jnp.where(row8 == i, q_two[base + i], two)
            last = jnp.where(row8 == i, q_last[base + i], last)
        return (
            jnp.where(live, obs - jnp.log(two), 0.0),
            jnp.where(live, obs - jnp.log(last), 0.0),
        )

    return final_rows


def scratch_for(total, width, people):
    return [
        pltpu.VMEM((width // LANES, total * 8, LANES), F32),
        pltpu.VMEM((people // LANES, total * 8, LANES), F32),
        pltpu.VMEM((GROUP, 48, width), F32),
        pltpu.VMEM((GROUP, 48, people), F32),
        pltpu.VMEM((GROUP, width, people), BF),
        pltpu.VMEM((GROUP // 2, people, 2 * width), BF),
        pltpu.VMEM((total, width), F32),
        pltpu.VMEM((total, 8, width), F32),
        pltpu.VMEM((total, 8, width), F32),
        pltpu.VMEM((total + 1, 8, width), F32),
        pltpu.VMEM((total + 1, 8, width), F32),
    ]


def early_markets(
    sigma, counts, converged, destination, start_offset, chars, share_rel, draws,
    *, devices, slots,
):
    total, width = start_offset.shape
    people = draws.shape[2]
    smem = pl.BlockSpec(memory_space=pltpu.SMEM)
    vmem = pl.BlockSpec(memory_space=pltpu.VMEM)
    hbm = pl.BlockSpec(memory_space=pltpu.HBM)
    return pl.pallas_call(
        functools.partial(early_kernel, slots=slots),
        out_shape=(
            jax.ShapeDtypeStruct((total, width), F32),
            jax.ShapeDtypeStruct((devices, 1, width + LANES), F32),
            jax.ShapeDtypeStruct((total,), jnp.int32),
        ),
        in_specs=[smem] * 4 + [hbm] * 4,
        out_specs=(vmem, vmem, smem),
        scratch_shapes=[
            pltpu.SMEM((2 * width // LANES,), jnp.int32),
            pltpu.VMEM(start_offset.shape, F32),
            pltpu.VMEM(chars.shape, F32),
            pltpu.VMEM(share_rel.shape, F32),
            pltpu.VMEM(draws.shape, F32),
            pltpu.SemaphoreType.DMA((4,)),
        ]
        + scratch_for(total, width, people),
        compiler_params=pltpu.CompilerParams(vmem_limit_bytes=60 * 2**20),
        name="early_markets",
    )(sigma, counts, converged, destination, start_offset, chars, share_rel, draws)


def late_markets(
    sigma, counts, converged, order, start_offset, chars, share_rel, draws, early
):
    total, width = start_offset.shape
    people = draws.shape[2]
    smem = pl.BlockSpec(memory_space=pltpu.SMEM)
    vmem = pl.BlockSpec(memory_space=pltpu.VMEM)
    rest = total - EARLY
    return pl.pallas_call(
        late_kernel,
        out_shape=jax.ShapeDtypeStruct((total, width), F32),
        in_specs=[smem] * 4 + [vmem] * 5,
        out_specs=vmem,
        scratch_shapes=[pltpu.SMEM((total,), jnp.int32)] + scratch_for(total, width, people),
        input_output_aliases={8: 0},
        compiler_params=pltpu.CompilerParams(vmem_limit_bytes=16 * 2**20),
        cost_estimate=pl.CostEstimate(
            flops=rest * width * people * 20,
            bytes_accessed=2 * 2**20,
            transcendentals=rest * width * people,
        ),
        name="late_markets",
    )(sigma, counts, converged, order, start_offset, chars, share_rel, draws, early)


def unpack_kernel(core, values, work, norm, *, cores):
    devices, _, width = values.shape
    width -= LANES
    slots = work.shape[0]
    row = lax.broadcasted_iota(jnp.int32, (slots, LANES), 0).astype(F32)
    acc = [jnp.zeros((slots, LANES), F32) for _ in range(width // LANES)]
    for chip in range(devices // cores):
        source = chip * cores + core[0]
        named = row == values[source, :, width : width + 1]
        for t in range(width // LANES):
            part = values[source, :, t * LANES : (t + 1) * LANES]
            acc[t] = jnp.where(named, jnp.broadcast_to(part, (slots, LANES)), acc[t])
    for t in range(width // LANES):
        work[:, t * LANES : (t + 1) * LANES] = acc[t]
    sums = [values[d, :, width:] for d in range(devices)]
    while len(sums) > 1:
        sums = [a + b for a, b in zip(sums[::2], sums[1::2])]
    norm[...] = jnp.sqrt(sums[0][:, 1:2] / sums[0][:, 2:3])


def unpack(core, values, cores, slots):
    devices, _, width = values.shape
    vmem = pl.BlockSpec(memory_space=pltpu.VMEM)
    return pl.pallas_call(
        functools.partial(unpack_kernel, cores=cores),
        out_shape=(
            jax.ShapeDtypeStruct((slots, width - LANES), F32),
            jax.ShapeDtypeStruct((1, 1), F32),
        ),
        in_specs=[pl.BlockSpec(memory_space=pltpu.SMEM), vmem],
        out_specs=(vmem, vmem),
        compiler_params=pltpu.CompilerParams(vmem_limit_bytes=4 * 2**20),
        name="unpack",
    )(core, values)


def local(start_offset, chars, share_rel, draws, sigma, counts, converged, destination):
    market_count, width = start_offset.shape
    devices = lax.axis_size(CHIP_CORES)
    slots = 3 * market_count // 8
    chars, draws = jnp.transpose(chars, (1, 0, 2)), jnp.transpose(draws, (1, 0, 2))
    early, send, order = early_markets(
        sigma, counts, converged, destination, start_offset, chars, share_rel, draws,
        devices=devices, slots=slots,
    )
    values = lax.all_to_all(send, CHIP_CORES, split_axis=0, concat_axis=0, tiled=True)
    delta = late_markets(
        sigma, counts, converged, order, start_offset, chars, share_rel, draws, early
    )
    work_delta, norm = unpack(
        jnp.full((1,), lax.axis_index("cores"), jnp.int32), values, lax.axis_size("cores"), slots
    )
    return delta, work_delta, norm[0, 0]


def solution(mesh):
    finer = Mesh(
        mesh.devices.reshape(4, 4, 2, mesh.shape["cores"]), ("chip_0", "chip_1", "chip_2", "cores")
    )
    row = P(CHIP_CORES)
    return jax.shard_map(
        local,
        mesh=finer,
        in_specs=(row, row, row, row, P(), row, row, row),
        out_specs=(row, row, P()),
        check_vma=False,
    )
```

```python
import functools
import math

import jax
import jax.numpy as jnp
from jax import lax
from jax.experimental import pallas as pl
from jax.experimental.pallas import tpu as pltpu
from jax.sharding import Mesh
from jax.sharding import PartitionSpec as P

TAIL_ITERS = 4
CHIP_CORES = ("chip_0", "chip_1", "chip_2", "cores")

SIDE = 256
GROUP = 4
EARLY = 20
LANES = 128
LOG2E = math.log2(math.e)
LIFT = 2.0**40
BF = jnp.bfloat16
F32 = jnp.float32


def three_parts(x):
    hi = x.astype(BF).astype(F32)
    mid = (x - hi).astype(BF).astype(F32)
    return hi, mid, x - hi - mid


def hi_lo_rows(x):
    hi = x.astype(BF).astype(F32)
    row = lax.broadcasted_iota(jnp.int32, x.shape, 0)
    return jnp.where(row < 4, hi, x - hi).astype(BF)


def add_halves(y):
    return y + pltpu.roll(y, 4, 0)


def by_turns(a, b):
    row = lax.broadcasted_iota(jnp.int32, a.shape, 0)
    return jnp.where(row % 2 == 0, a, b)


def dot(a, b):
    return jnp.dot(a, b, preferred_element_type=F32)


def sort_markets(counts, converged, order, bucket_at, total, tiles):
    def bucket(i):
        return converged[i] * tiles + (tiles - (counts[i] + LANES - 1) // LANES)

    for b in range(2 * tiles):
        bucket_at[b] = 0

    def tally(i, active):
        b = bucket(i)
        bucket_at[b] = bucket_at[b] + 1
        return active + jnp.where(converged[i] == 0, counts[i], 0)

    active = lax.fori_loop(0, total, tally, jnp.int32(0), unroll=True)
    at = jnp.int32(0)
    for b in range(2 * tiles):
        size = bucket_at[b]
        bucket_at[b] = at
        at = at + size

    def put(i, _):
        b = bucket(i)
        order[bucket_at[b]] = i
        bucket_at[b] = bucket_at[b] + 1
        return 0

    lax.fori_loop(0, total, put, 0, unroll=True)
    return active


def early_kernel(
    sigma, counts, converged, destination, start, chars, share, draws,
    delta, send, order,
    bucket_at, start_here, chars_here, share_here, draws_here, copied, *scratch, slots,
):
    total, width = start.shape
    copies = [
        pltpu.make_async_copy(source, here, copied.at[i])
        for i, (source, here) in enumerate(
            ((start, start_here), (share, share_here), (chars, chars_here), (draws, draws_here))
        )
    ]
    for copy in copies:
        copy.start()

    def ready(which):
        for copy in copies[which]:
            copy.wait()

    active = sort_markets(counts, converged, order, bucket_at, total, width // LANES)
    final_rows = run_markets(
        sigma, counts, converged, start_here, chars_here, share_here, draws_here, order, *scratch,
        0, EARLY, ready,
    )
    row8 = lax.broadcasted_iota(jnp.int32, (8, width), 0)
    acc = jnp.zeros((8, width), F32)
    for base in range(0, total, 8):
        two, last = final_rows(base)
        delta[pl.ds(base, 8), :] = last
        done = jnp.ones((8, width), jnp.int32)
        for i in range(8):
            done = jnp.where(row8 == i, converged[base + i], done)
        step = jnp.where(done == 0, last - two, 0.0)
        acc = acc + step * step

    change = jnp.sum(jnp.sum(acc, axis=1, keepdims=True), axis=0, keepdims=True)
    side = lax.broadcasted_iota(jnp.int32, (1, LANES), 1)
    empty = jnp.where(side == 1, change, jnp.where(side == 2, active.astype(F32), float(slots)))
    for c in range(send.shape[0]):
        send[c, :, width:] = empty
    for i in range(total):

        @pl.when(converged[i] == 0)
        def _():
            device = destination[i] // slots
            slot = (destination[i] % slots).astype(F32)
            send[device, :, :width] = delta[i : i + 1, :]
            send[device, :, width:] = jnp.where(side == 0, slot, empty)


def late_kernel(
    sigma, counts, converged, order, start, chars, share, draws, early,
    delta,
    late, *scratch,
):
    total, width = start.shape
    final_rows = run_markets(
        sigma, counts, converged, start, chars, share, draws, order, *scratch, EARLY, total
    )
    for i in range(total):
        late[order[i]] = 1 if i >= EARLY else 0
    row8 = lax.broadcasted_iota(jnp.int32, (8, width), 0)
    for base in range(0, total, 8):
        rows = pl.ds(base, 8)
        here = jnp.zeros((8, width), jnp.int32)
        for i in range(8):
            here = jnp.where(row8 == i, late[base + i], here)
        delta[rows, :] = jnp.where(here == 1, final_rows(base)[1], early[rows, :])


def run_markets(
    sigma, counts, converged, start, chars, share, draws, order,
    chars_rows, draws_rows, a_stack, b_stack, table, table_t, log_obs, goal, first, q_two, q_last,
    begin, end, ready=lambda which: None,
):
    total, width = start.shape
    people = draws.shape[2]
    k_count = chars.shape[0]
    tiles = width // LANES
    scale = LIFT * people

    row8 = lax.broadcasted_iota(jnp.int32, (8, width), 0)
    lane = lax.broadcasted_iota(jnp.int32, (8, width), 1)
    lives = []
    ready(slice(0, 2))
    for base in range(0, total, 8):
        count = jnp.zeros((8, width), jnp.int32)
        for i in range(8):
            count = jnp.where(row8 == i, counts[base + i], count)
        live = lane < count
        lives.append(live)
        rows = pl.ds(base, 8)
        obs = share[rows, :] - jnp.log(count.astype(F32)) - 1.5
        log_obs[rows, :] = obs
        wanted = jnp.where(live, jnp.exp(obs) * scale, 0.0)
        opening = jnp.where(live, jnp.exp(obs + start[rows, :]), 0.0)
        for i in range(8):
            goal[base + i] = jnp.broadcast_to(wanted[i : i + 1], (8, width))
            first[base + i] = jnp.broadcast_to(opening[i : i + 1], (8, width))

    coef = jnp.zeros((8, width), F32)
    for k in range(k_count):
        coef = jnp.where(row8 == k, sigma[k] * LOG2E, coef)
    ready(slice(2, 4))
    for source, rows in ((chars, chars_rows), (draws, draws_rows)):
        rows[...] = jnp.zeros(rows.shape, F32)
        for k in range(k_count):
            for base in range(0, total, 8):
                for t in range(rows.shape[0]):
                    part = source[k, base : base + 8, t * LANES : (t + 1) * LANES]
                    rows[t, pl.ds(base * 8 + k, 8, stride=8), :] = part

    def put_stack(ref, g, parts):
        for i, part in enumerate(parts):
            ref[g, 8 * i : 8 * i + 8, : part.shape[1]] = part

    def build(n, market, g):
        rows = pl.ds(pl.multiple_of(market * 8, 8), 8)
        a = jnp.concatenate([chars_rows[t, rows, :] for t in range(n // LANES)], axis=1)
        b = jnp.concatenate([draws_rows[t, rows, :] for t in range(people // LANES)], axis=1)
        a1, a2, a3 = three_parts(a * coef[:, :n])
        b1, b2, b3 = three_parts(b)
        put_stack(a_stack, g, (a1, a1, a2, a1, a2, a3))
        put_stack(b_stack, g, (b1, b2, b1, b3, b2, b1))
        a_t = jnp.transpose(a_stack[g, :, :n], (1, 0)).astype(BF)
        t = jnp.exp2(dot(a_t, b_stack[g].astype(BF))).astype(BF)
        table[g, :n, :] = t
        at = (g % 2) * n
        table_t[g // 2, :, at : at + n] = jnp.transpose(t, (1, 0))

    def run_group(n, base):
        ids = [order[base + g] for g in range(GROUP)]
        busy = [1 - converged[i] for i in ids]
        trips = 1 + TAIL_ITERS // 2 * functools.reduce(jnp.maximum, busy)
        for g in range(GROUP):
            build(n, ids[g], g)
        pairs = range(GROUP // 2)
        by_matrix = people - SIDE
        goals = [by_turns(goal[ids[2 * p], :, :n], goal[ids[2 * p + 1], :, :n]) for p in pairs]
        firsts = [by_turns(first[ids[2 * p], :, :n], first[ids[2 * p + 1], :, :n]) for p in pairs]

        def step(state):
            weights = []
            sides = []
            for p in pairs:
                e = hi_lo_rows(state[p])
                inside = by_turns(dot(e, table[2 * p, :n, :]), dot(e, table[2 * p + 1, :n, :]))
                weight = LIFT / (1.0 + add_halves(inside))
                weights.append(hi_lo_rows(weight[:, :by_matrix]))
                sides.append([side_sum(p, h, n, weight) for h in range(2)])
            sums = []
            for p in pairs:
                y = dot(weights[p], table_t[p, :by_matrix, : 2 * n])
                y = by_turns(y[:, :n] + sides[p][0], y[:, n:] + sides[p][1])
                sums.append(add_halves(y))
            return sums

        def side_sum(p, h, n, weight):
            total8 = jnp.zeros((8, n), F32)
            for r0 in range(by_matrix, people, LANES):
                row = jnp.broadcast_to(weight[h : h + 1, r0 : r0 + LANES], (LANES, LANES))
                column = jnp.transpose(row, (1, 0))
                block = table_t[p, r0 : r0 + LANES, h * n : (h + 1) * n].astype(F32)
                for r in range(0, LANES, 8):
                    w = column[r : r + 8]
                    w = jnp.concatenate([w] * (n // LANES), axis=1)
                    total8 = total8 + block[r : r + 8] * w
            total8 = total8 + pltpu.roll(total8, 2, 0)
            return total8 + pltpu.roll(total8, 1, 0)

        def two_steps(trip, state):
            sums = step(state)
            sums = step([goals[p] / sums[p] for p in pairs])
            for p in pairs:
                q = sums[p]
                other = pltpu.roll(q, 1, 0)
                for g, rows in ((2 * p, by_turns(q, other)), (2 * p + 1, by_turns(other, q))):
                    q_two[jnp.where(trip == 0, ids[g], total), :, :n] = rows
                    keep = jnp.logical_or(trip == 0, busy[g] == 1)
                    q_last[jnp.where(keep, ids[g], total), :, :n] = rows
            return tuple(goals[p] / sums[p] for p in pairs)

        lax.fori_loop(0, trips, two_steps, tuple(firsts))

    def one_group(j, _):
        base = j * GROUP
        size = counts[order[base]]
        for g in range(1, GROUP):
            size = jnp.maximum(size, counts[order[base + g]])
        for t in range(1, tiles + 1):

            @pl.when((size + LANES - 1) // LANES == t)
            def _():
                run_group(t * LANES, base)

        return 0

    lax.fori_loop(begin // GROUP, end // GROUP, one_group, 0)

    def final_rows(base):
        obs = log_obs[pl.ds(base, 8), :] + math.log(scale)
        live = lives[base // 8]
        two = q_two[base]
        last = q_last[base]
        for i in range(1, 8):
            two = jnp.where(row8 == i, q_two[base + i], two)
            last = jnp.where(row8 == i, q_last[base + i], last)
        return (
            jnp.where(live, obs - jnp.log(two), 0.0),
            jnp.where(live, obs - jnp.log(last), 0.0),
        )

    return final_rows


def scratch_for(total, width, people):
    return [
        pltpu.VMEM((width // LANES, total * 8, LANES), F32),
        pltpu.VMEM((people // LANES, total * 8, LANES), F32),
        pltpu.VMEM((GROUP, 48, width), F32),
        pltpu.VMEM((GROUP, 48, people), F32),
        pltpu.VMEM((GROUP, width, people), BF),
        pltpu.VMEM((GROUP // 2, people, 2 * width), BF),
        pltpu.VMEM((total, width), F32),
        pltpu.VMEM((total, 8, width), F32),
        pltpu.VMEM((total, 8, width), F32),
        pltpu.VMEM((total + 1, 8, width), F32),
        pltpu.VMEM((total + 1, 8, width), F32),
    ]


def early_markets(
    sigma, counts, converged, destination, start_offset, chars, share_rel, draws,
    *, devices, slots,
):
    total, width = start_offset.shape
    people = draws.shape[2]
    smem = pl.BlockSpec(memory_space=pltpu.SMEM)
    vmem = pl.BlockSpec(memory_space=pltpu.VMEM)
    hbm = pl.BlockSpec(memory_space=pltpu.HBM)
    return pl.pallas_call(
        functools.partial(early_kernel, slots=slots),
        out_shape=(
            jax.ShapeDtypeStruct((total, width), F32),
            jax.ShapeDtypeStruct((devices, 1, width + LANES), F32),
            jax.ShapeDtypeStruct((total,), jnp.int32),
        ),
        in_specs=[smem] * 4 + [hbm] * 4,
        out_specs=(vmem, vmem, smem),
        scratch_shapes=[
            pltpu.SMEM((2 * width // LANES,), jnp.int32),
            pltpu.VMEM(start_offset.shape, F32),
            pltpu.VMEM(chars.shape, F32),
            pltpu.VMEM(share_rel.shape, F32),
            pltpu.VMEM(draws.shape, F32),
            pltpu.SemaphoreType.DMA((4,)),
        ]
        + scratch_for(total, width, people),
        compiler_params=pltpu.CompilerParams(vmem_limit_bytes=60 * 2**20),
        name="early_markets",
    )(sigma, counts, converged, destination, start_offset, chars, share_rel, draws)


def late_markets(
    sigma, counts, converged, order, start_offset, chars, share_rel, draws, early
):
    total, width = start_offset.shape
    people = draws.shape[2]
    smem = pl.BlockSpec(memory_space=pltpu.SMEM)
    vmem = pl.BlockSpec(memory_space=pltpu.VMEM)
    rest = total - EARLY
    return pl.pallas_call(
        late_kernel,
        out_shape=jax.ShapeDtypeStruct((total, width), F32),
        in_specs=[smem] * 4 + [vmem] * 5,
        out_specs=vmem,
        scratch_shapes=[pltpu.SMEM((total,), jnp.int32)] + scratch_for(total, width, people),
        input_output_aliases={8: 0},
        compiler_params=pltpu.CompilerParams(vmem_limit_bytes=16 * 2**20),
        cost_estimate=pl.CostEstimate(
            flops=rest * width * people * 20,
            bytes_accessed=2 * 2**20,
            transcendentals=rest * width * people,
        ),
        name="late_markets",
    )(sigma, counts, converged, order, start_offset, chars, share_rel, draws, early)


def unpack_kernel(core, values, work, norm, *, cores):
    devices, _, width = values.shape
    width -= LANES
    slots = work.shape[0]
    row = lax.broadcasted_iota(jnp.int32, (slots, LANES), 0).astype(F32)
    acc = [jnp.zeros((slots, LANES), F32) for _ in range(width // LANES)]
    for chip in range(devices // cores):
        source = chip * cores + core[0]
        named = row == values[source, :, width : width + 1]
        for t in range(width // LANES):
            part = values[source, :, t * LANES : (t + 1) * LANES]
            acc[t] = jnp.where(named, jnp.broadcast_to(part, (slots, LANES)), acc[t])
    for t in range(width // LANES):
        work[:, t * LANES : (t + 1) * LANES] = acc[t]
    sums = [values[d, :, width:] for d in range(devices)]
    while len(sums) > 1:
        sums = [a + b for a, b in zip(sums[::2], sums[1::2])]
    norm[...] = jnp.sqrt(sums[0][:, 1:2] / sums[0][:, 2:3])


def unpack(core, values, cores, slots):
    devices, _, width = values.shape
    vmem = pl.BlockSpec(memory_space=pltpu.VMEM)
    return pl.pallas_call(
        functools.partial(unpack_kernel, cores=cores),
        out_shape=(
            jax.ShapeDtypeStruct((slots, width - LANES), F32),
            jax.ShapeDtypeStruct((1, 1), F32),
        ),
        in_specs=[pl.BlockSpec(memory_space=pltpu.SMEM), vmem],
        out_specs=(vmem, vmem),
        compiler_params=pltpu.CompilerParams(vmem_limit_bytes=4 * 2**20),
        name="unpack",
    )(core, values)


def local(start_offset, chars, share_rel, draws, sigma, counts, converged, destination):
    market_count, width = start_offset.shape
    devices = lax.axis_size(CHIP_CORES)
    slots = 3 * market_count // 8
    chars, draws = jnp.transpose(chars, (1, 0, 2)), jnp.transpose(draws, (1, 0, 2))
    early, send, order = early_markets(
        sigma, counts, converged, destination, start_offset, chars, share_rel, draws,
        devices=devices, slots=slots,
    )
    values = lax.all_to_all(send, CHIP_CORES, split_axis=0, concat_axis=0, tiled=True)
    delta = late_markets(
        sigma, counts, converged, order, start_offset, chars, share_rel, draws, early
    )
    work_delta, norm = unpack(
        jnp.full((1,), lax.axis_index("cores"), jnp.int32), values, lax.axis_size("cores"), slots
    )
    return delta, work_delta, norm[0, 0]


def solution(mesh):
    finer = Mesh(
        mesh.devices.reshape(4, 4, 2, mesh.shape["cores"]), ("chip_0", "chip_1", "chip_2", "cores")
    )
    row = P(CHIP_CORES)
    return jax.shard_map(
        local,
        mesh=finer,
        in_specs=(row, row, row, row, P(), row, row, row),
        out_specs=(row, row, P()),
        check_vma=False,
    )
```

```python
import functools
import math

import jax
import jax.numpy as jnp
from jax import lax
from jax.experimental import pallas as pl
from jax.experimental.pallas import tpu as pltpu
from jax.sharding import Mesh
from jax.sharding import PartitionSpec as P

TAIL_ITERS = 4
CHIP_CORES = ("chip_0", "chip_1", "chip_2", "cores")

SIDE = 256
GROUP = 4
EARLY = 20
LANES = 128
LOG2E = math.log2(math.e)
LIFT = 2.0**40
BF = jnp.bfloat16
F32 = jnp.float32


def three_parts(x):
    hi = x.astype(BF).astype(F32)
    mid = (x - hi).astype(BF).astype(F32)
    return hi, mid, x - hi - mid


def hi_lo_rows(x):
    hi = x.astype(BF).astype(F32)
    row = lax.broadcasted_iota(jnp.int32, x.shape, 0)
    return jnp.where(row < 4, hi, x - hi).astype(BF)


def add_halves(y):
    return y + pltpu.roll(y, 4, 0)


def by_turns(a, b):
    row = lax.broadcasted_iota(jnp.int32, a.shape, 0)
    return jnp.where(row % 2 == 0, a, b)


def dot(a, b):
    return jnp.dot(a, b, preferred_element_type=F32)


def sort_markets(counts, converged, order, bucket_at, total, tiles):
    def bucket(i):
        return converged[i] * tiles + (tiles - (counts[i] + LANES - 1) // LANES)

    for b in range(2 * tiles):
        bucket_at[b] = 0

    def tally(i, active):
        b = bucket(i)
        bucket_at[b] = bucket_at[b] + 1
        return active + jnp.where(converged[i] == 0, counts[i], 0)

    active = lax.fori_loop(0, total, tally, jnp.int32(0), unroll=True)
    at = jnp.int32(0)
    for b in range(2 * tiles):
        size = bucket_at[b]
        bucket_at[b] = at
        at = at + size

    def put(i, _):
        b = bucket(i)
        order[bucket_at[b]] = i
        bucket_at[b] = bucket_at[b] + 1
        return 0

    lax.fori_loop(0, total, put, 0, unroll=True)
    return active


def early_kernel(
    sigma, counts, converged, destination, start, chars, share, draws,
    delta, send, order,
    bucket_at, start_here, chars_here, share_here, draws_here, copied, *scratch, slots,
):
    total, width = start.shape
    copies = [
        pltpu.make_async_copy(source, here, copied.at[i])
        for i, (source, here) in enumerate(
            ((start, start_here), (share, share_here), (chars, chars_here), (draws, draws_here))
        )
    ]
    for copy in copies:
        copy.start()

    def ready(which):
        for copy in copies[which]:
            copy.wait()

    active = sort_markets(counts, converged, order, bucket_at, total, width // LANES)
    final_rows = run_markets(
        sigma, counts, converged, start_here, chars_here, share_here, draws_here, order, *scratch,
        0, EARLY, True, ready,
    )
    row8 = lax.broadcasted_iota(jnp.int32, (8, width), 0)
    acc = jnp.zeros((8, width), F32)
    for base in range(0, total, 8):
        two, last = final_rows(base)
        delta[pl.ds(base, 8), :] = last
        done = jnp.ones((8, width), jnp.int32)
        for i in range(8):
            done = jnp.where(row8 == i, converged[base + i], done)
        step = jnp.where(done == 0, last - two, 0.0)
        acc = acc + step * step

    change = jnp.sum(jnp.sum(acc, axis=1, keepdims=True), axis=0, keepdims=True)
    side = lax.broadcasted_iota(jnp.int32, (1, LANES), 1)
    empty = jnp.where(side == 1, change, jnp.where(side == 2, active.astype(F32), float(slots)))
    for c in range(send.shape[0]):
        send[c, :, width:] = empty
    for i in range(total):

        @pl.when(converged[i] == 0)
        def _():
            device = destination[i] // slots
            slot = (destination[i] % slots).astype(F32)
            send[device, :, :width] = delta[i : i + 1, :]
            send[device, :, width:] = jnp.where(side == 0, slot, empty)


def late_kernel(
    sigma, counts, converged, order, start, chars, share, draws, early,
    delta,
    late, *scratch,
):
    total, width = start.shape
    final_rows = run_markets(
        sigma, counts, converged, start, chars, share, draws, order, *scratch, EARLY, total
    )
    for i in range(total):
        late[order[i]] = 1 if i >= EARLY else 0
    row8 = lax.broadcasted_iota(jnp.int32, (8, width), 0)
    for base in range(0, total, 8):
        rows = pl.ds(base, 8)
        here = jnp.zeros((8, width), jnp.int32)
        for i in range(8):
            here = jnp.where(row8 == i, late[base + i], here)
        delta[rows, :] = jnp.where(here == 1, final_rows(base)[1], early[rows, :])


def run_markets(
    sigma, counts, converged, start, chars, share, draws, order,
    chars_rows, draws_rows, a_stack, b_stack, table, table_t, log_obs, goal, first, q_two, q_last,
    begin, end, tail=False, ready=lambda which: None,
):
    total, width = start.shape
    people = draws.shape[2]
    k_count = chars.shape[0]
    tiles = width // LANES
    scale = LIFT * people

    row8 = lax.broadcasted_iota(jnp.int32, (8, width), 0)
    lane = lax.broadcasted_iota(jnp.int32, (8, width), 1)
    lives = []
    ready(slice(0, 2))
    for base in range(0, total, 8):
        count = jnp.zeros((8, width), jnp.int32)
        for i in range(8):
            count = jnp.where(row8 == i, counts[base + i], count)
        live = lane < count
        lives.append(live)
        rows = pl.ds(base, 8)
        obs = share[rows, :] - jnp.log(count.astype(F32)) - 1.5
        log_obs[rows, :] = obs
        wanted = jnp.where(live, jnp.exp(obs) * scale, 0.0)
        opening = jnp.where(live, jnp.exp(obs + start[rows, :]), 0.0)
        for i in range(8):
            goal[base + i] = jnp.broadcast_to(wanted[i : i + 1], (8, width))
            first[base + i] = jnp.broadcast_to(opening[i : i + 1], (8, width))

    coef = jnp.zeros((8, width), F32)
    for k in range(k_count):
        coef = jnp.where(row8 == k, sigma[k] * LOG2E, coef)
    ready(slice(2, 4))
    for source, rows in ((chars, chars_rows), (draws, draws_rows)):
        rows[...] = jnp.zeros(rows.shape, F32)
        for k in range(k_count):
            for base in range(0, total, 8):
                for t in range(rows.shape[0]):
                    part = source[k, base : base + 8, t * LANES : (t + 1) * LANES]
                    rows[t, pl.ds(base * 8 + k, 8, stride=8), :] = part

    def put_stack(ref, g, parts):
        for i, part in enumerate(parts):
            ref[g, 8 * i : 8 * i + 8, : part.shape[1]] = part

    def build(n, market, g):
        rows = pl.ds(pl.multiple_of(market * 8, 8), 8)
        a = jnp.concatenate([chars_rows[t, rows, :] for t in range(n // LANES)], axis=1)
        b = jnp.concatenate([draws_rows[t, rows, :] for t in range(people // LANES)], axis=1)
        a1, a2, a3 = three_parts(a * coef[:, :n])
        b1, b2, b3 = three_parts(b)
        put_stack(a_stack, g, (a1, a1, a2, a1, a2, a3))
        put_stack(b_stack, g, (b1, b2, b1, b3, b2, b1))
        a_t = jnp.transpose(a_stack[g, :, :n], (1, 0)).astype(BF)
        t = jnp.exp2(dot(a_t, b_stack[g].astype(BF))).astype(BF)
        table[g, :n, :] = t
        at = (g % 2) * n
        table_t[g // 2, :, at : at + n] = jnp.transpose(t, (1, 0))

    def run_group(n, base):
        ids = [order[base + g] for g in range(GROUP)]
        busy = [1 - converged[i] for i in ids]
        for g in range(GROUP):
            build(n, ids[g], g)
        pairs = range(GROUP // 2)
        by_matrix = people - SIDE
        goals = [by_turns(goal[ids[2 * p], :, :n], goal[ids[2 * p + 1], :, :n]) for p in pairs]
        firsts = [by_turns(first[ids[2 * p], :, :n], first[ids[2 * p + 1], :, :n]) for p in pairs]

        def step(state):
            weights = []
            sides = []
            for p in pairs:
                e = hi_lo_rows(state[p])
                inside = by_turns(dot(e, table[2 * p, :n, :]), dot(e, table[2 * p + 1, :n, :]))
                weight = LIFT / (1.0 + add_halves(inside))
                weights.append(hi_lo_rows(weight[:, :by_matrix]))
                sides.append([side_sum(p, h, n, weight) for h in range(2)])
            sums = []
            for p in pairs:
                y = dot(weights[p], table_t[p, :by_matrix, : 2 * n])
                y = by_turns(y[:, :n] + sides[p][0], y[:, n:] + sides[p][1])
                sums.append(add_halves(y))
            return sums

        def side_sum(p, h, n, weight):
            total8 = jnp.zeros((8, n), F32)
            for r0 in range(by_matrix, people, LANES):
                row = jnp.broadcast_to(weight[h : h + 1, r0 : r0 + LANES], (LANES, LANES))
                column = jnp.transpose(row, (1, 0))
                block = table_t[p, r0 : r0 + LANES, h * n : (h + 1) * n].astype(F32)
                for r in range(0, LANES, 8):
                    w = column[r : r + 8]
                    w = jnp.concatenate([w] * (n // LANES), axis=1)
                    total8 = total8 + block[r : r + 8] * w
            total8 = total8 + pltpu.roll(total8, 2, 0)
            return total8 + pltpu.roll(total8, 1, 0)

        def steps(count, state):
            for it in range(count):
                sums = step(state)
                state = [goals[p] / sums[p] for p in pairs]
            rows = []
            for q in sums:
                other = pltpu.roll(q, 1, 0)
                rows += [by_turns(q, other), by_turns(other, q)]
            return state, rows

        state, rows = steps(2, firsts)
        for g in range(GROUP):
            q_two[ids[g], :, :n] = rows[g]
            q_last[ids[g], :, :n] = rows[g]
        if not tail:
            return

        @pl.when(functools.reduce(jnp.maximum, busy) == 1)
        def _():
            _, rows = steps(TAIL_ITERS, state)
            for g in range(GROUP):
                q_last[jnp.where(busy[g] == 1, ids[g], total), :, :n] = rows[g]

    def one_group(j, _):
        base = j * GROUP
        size = counts[order[base]]
        for g in range(1, GROUP):
            size = jnp.maximum(size, counts[order[base + g]])
        for t in range(1, tiles + 1):

            @pl.when((size + LANES - 1) // LANES == t)
            def _():
                run_group(t * LANES, base)

        return 0

    lax.fori_loop(begin // GROUP, end // GROUP, one_group, 0)

    def final_rows(base):
        obs = log_obs[pl.ds(base, 8), :] + math.log(scale)
        live = lives[base // 8]
        two = q_two[base]
        last = q_last[base]
        for i in range(1, 8):
            two = jnp.where(row8 == i, q_two[base + i], two)
            last = jnp.where(row8 == i, q_last[base + i], last)
        return (
            jnp.where(live, obs - jnp.log(two), 0.0),
            jnp.where(live, obs - jnp.log(last), 0.0),
        )

    return final_rows


def scratch_for(total, width, people):
    return [
        pltpu.VMEM((width // LANES, total * 8, LANES), F32),
        pltpu.VMEM((people // LANES, total * 8, LANES), F32),
        pltpu.VMEM((GROUP, 48, width), F32),
        pltpu.VMEM((GROUP, 48, people), F32),
        pltpu.VMEM((GROUP, width, people), BF),
        pltpu.VMEM((GROUP // 2, people, 2 * width), BF),
        pltpu.VMEM((total, width), F32),
        pltpu.VMEM((total, 8, width), F32),
        pltpu.VMEM((total, 8, width), F32),
        pltpu.VMEM((total + 1, 8, width), F32),
        pltpu.VMEM((total + 1, 8, width), F32),
    ]


def early_markets(
    sigma, counts, converged, destination, start_offset, chars, share_rel, draws,
    *, devices, slots,
):
    total, width = start_offset.shape
    people = draws.shape[2]
    smem = pl.BlockSpec(memory_space=pltpu.SMEM)
    vmem = pl.BlockSpec(memory_space=pltpu.VMEM)
    hbm = pl.BlockSpec(memory_space=pltpu.HBM)
    return pl.pallas_call(
        functools.partial(early_kernel, slots=slots),
        out_shape=(
            jax.ShapeDtypeStruct((total, width), F32),
            jax.ShapeDtypeStruct((devices, 1, width + LANES), F32),
            jax.ShapeDtypeStruct((total,), jnp.int32),
        ),
        in_specs=[smem] * 4 + [hbm] * 4,
        out_specs=(vmem, vmem, smem),
        scratch_shapes=[
            pltpu.SMEM((2 * width // LANES,), jnp.int32),
            pltpu.VMEM(start_offset.shape, F32),
            pltpu.VMEM(chars.shape, F32),
            pltpu.VMEM(share_rel.shape, F32),
            pltpu.VMEM(draws.shape, F32),
            pltpu.SemaphoreType.DMA((4,)),
        ]
        + scratch_for(total, width, people),
        compiler_params=pltpu.CompilerParams(vmem_limit_bytes=60 * 2**20),
        name="early_markets",
    )(sigma, counts, converged, destination, start_offset, chars, share_rel, draws)


def late_markets(
    sigma, counts, converged, order, start_offset, chars, share_rel, draws, early
):
    total, width = start_offset.shape
    people = draws.shape[2]
    smem = pl.BlockSpec(memory_space=pltpu.SMEM)
    vmem = pl.BlockSpec(memory_space=pltpu.VMEM)
    rest = total - EARLY
    return pl.pallas_call(
        late_kernel,
        out_shape=jax.ShapeDtypeStruct((total, width), F32),
        in_specs=[smem] * 4 + [vmem] * 5,
        out_specs=vmem,
        scratch_shapes=[pltpu.SMEM((total,), jnp.int32)] + scratch_for(total, width, people),
        input_output_aliases={8: 0},
        compiler_params=pltpu.CompilerParams(vmem_limit_bytes=16 * 2**20),
        cost_estimate=pl.CostEstimate(
            flops=rest * width * people * 20,
            bytes_accessed=2 * 2**20,
            transcendentals=rest * width * people,
        ),
        name="late_markets",
    )(sigma, counts, converged, order, start_offset, chars, share_rel, draws, early)


def unpack_kernel(core, values, work, norm, *, cores):
    devices, _, width = values.shape
    width -= LANES
    slots = work.shape[0]
    row = lax.broadcasted_iota(jnp.int32, (slots, LANES), 0).astype(F32)
    acc = [jnp.zeros((slots, LANES), F32) for _ in range(width // LANES)]
    for chip in range(devices // cores):
        source = chip * cores + core[0]
        named = row == values[source, :, width : width + 1]
        for t in range(width // LANES):
            part = values[source, :, t * LANES : (t + 1) * LANES]
            acc[t] = jnp.where(named, jnp.broadcast_to(part, (slots, LANES)), acc[t])
    for t in range(width // LANES):
        work[:, t * LANES : (t + 1) * LANES] = acc[t]
    sums = [values[d, :, width:] for d in range(devices)]
    while len(sums) > 1:
        sums = [a + b for a, b in zip(sums[::2], sums[1::2])]
    norm[...] = jnp.sqrt(sums[0][:, 1:2] / sums[0][:, 2:3])


def unpack(core, values, cores, slots):
    devices, _, width = values.shape
    vmem = pl.BlockSpec(memory_space=pltpu.VMEM)
    return pl.pallas_call(
        functools.partial(unpack_kernel, cores=cores),
        out_shape=(
            jax.ShapeDtypeStruct((slots, width - LANES), F32),
            jax.ShapeDtypeStruct((1, 1), F32),
        ),
        in_specs=[pl.BlockSpec(memory_space=pltpu.SMEM), vmem],
        out_specs=(vmem, vmem),
        compiler_params=pltpu.CompilerParams(vmem_limit_bytes=4 * 2**20),
        name="unpack",
    )(core, values)


def local(start_offset, chars, share_rel, draws, sigma, counts, converged, destination):
    market_count, width = start_offset.shape
    devices = lax.axis_size(CHIP_CORES)
    slots = 3 * market_count // 8
    chars, draws = jnp.transpose(chars, (1, 0, 2)), jnp.transpose(draws, (1, 0, 2))
    early, send, order = early_markets(
        sigma, counts, converged, destination, start_offset, chars, share_rel, draws,
        devices=devices, slots=slots,
    )
    values = lax.all_to_all(send, CHIP_CORES, split_axis=0, concat_axis=0, tiled=True)
    delta = late_markets(
        sigma, counts, converged, order, start_offset, chars, share_rel, draws, early
    )
    work_delta, norm = unpack(
        jnp.full((1,), lax.axis_index("cores"), jnp.int32), values, lax.axis_size("cores"), slots
    )
    return delta, work_delta, norm[0, 0]


def solution(mesh):
    finer = Mesh(
        mesh.devices.reshape(4, 4, 2, mesh.shape["cores"]), ("chip_0", "chip_1", "chip_2", "cores")
    )
    row = P(CHIP_CORES)
    return jax.shard_map(
        local,
        mesh=finer,
        in_specs=(row, row, row, row, P(), row, row, row),
        out_specs=(row, row, P()),
        check_vma=False,
    )
```
